32 devices in a mesh: dp: 16 (over z, y, core), tensor: 2 (over x).
Axes of the slice: x: 2, y: 2, z: 4, core: 2. Of those that a mesh axis runs over, the one named last changes fastest.
Arguments:
- attn_out: bfloat16 [12288, 2048], P('dp', 'tensor'), may hold values from -6 to 6
- out_proj_t: bfloat16 [4096, 2048], P(None, 'tensor'), may hold values from -0.09375 to 0.09375
- grad_out: bfloat16 [12288, 4096], P('dp', 'tensor'), may hold values from -6 to 6
- read_weights: float32 [12288, 16], P('dp'), may hold values from 0 to 0.0026041667
- memory_gate: float32 [256, 16], P('dp'), may hold values from -0.2 to 1
- write_pos: int32 [16, 16], P('dp'), may hold values from 0 to 767, as said below
Outputs:
- grad_attn_out: bfloat16 [12288, 2048], P('dp', 'tensor')
- grad_out_proj_t: float32 [4096, 2048], P('dp', 'tensor')
- grad_memory: float32 [256, 4096], P('dp', 'tensor')
The draws below stay inside these ranges and needn't reach their ends.
Inputs may be any that keep to these rules, and one draw needn't show every extreme that they name: `write_pos`: the 16 positions of one segment are distinct.
All inputs are finite; a program needn't handle non-finite values.
Results may differ from the reference program's by a relative error of at most 0.0034.
Values may be sent and summed in bfloat16 or wider, within the bound.
No kernel may reach another device: no remote copies, remote signals or barrier semaphores. Data moves between devices by JAX's collectives and lax.ppermute only.
A program may use at most 64 MiB of HBM per device.

```python
import jax
import jax.numpy as jnp
from jax import lax

D = 4096
MEM = 16
SEG = 768
SEGMENT_COUNT = 16
HD = 2048
TOKENS = 12288


def draw_memory_gate(key, part):
    share = 0.5
    gradual_decay = jax.random.uniform(jax.random.fold_in(key, 1), (1, MEM)) < share
    gradual_decay_rate = jnp.exp(-jax.random.uniform(jax.random.fold_in(key, 2), (SEGMENT_COUNT, MEM), jnp.float32, 0.2, 1.5) / SEGMENT_COUNT)
    quick_decay_rate = jax.random.uniform(jax.random.fold_in(key, 3), (SEGMENT_COUNT, MEM), jnp.float32, 0.05, 0.5)
    sudden_spike = jax.random.uniform(jax.random.fold_in(key, 4), (SEGMENT_COUNT, 1)) < 3.0 / SEGMENT_COUNT
    decay_rates = jnp.where(gradual_decay, gradual_decay_rate, quick_decay_rate) * jnp.where(sudden_spike, 0.6, 1.0)
    eye = jnp.eye(MEM, dtype=jnp.float32)
    spread = jnp.clip(jax.random.normal(jax.random.fold_in(key, 5), (SEGMENT_COUNT, MEM, MEM)) * 0.04, -0.2, 0.2)
    gates = spread * (1.0 - eye) + decay_rates[:, :, None] * eye
    return gates.reshape(SEGMENT_COUNT * MEM, MEM).astype(jnp.float32)


def draw_write_pos(key, part):
    keys = jax.random.split(jax.random.fold_in(key, 7), SEGMENT_COUNT)
    picks = jax.vmap(lambda single: jax.random.permutation(single, SEG)[:MEM])(keys)
    return picks.astype(jnp.int32)


def spiked(drawn, stream_key, source, target, parts, factor):
    def block_of(position):
        return (jnp.arange(drawn.shape[position]) // (drawn.shape[position] // parts)).reshape((-1,) + (1,) * (drawn.ndim - 1 - position))

    one_side = jax.random.permutation(stream_key, parts)[block_of(target)]
    second = (block_of(target) + parts // 2) % parts
    return jnp.where((block_of(source) == one_side) | (block_of(source) == second), factor * drawn, drawn)


def levels(rng, dims, cuts, low, high):
    def one(dim, shards_of):
        steps = jax.random.uniform(jax.random.fold_in(jax.random.fold_in(rng, 6), dim), (shards_of,), jnp.float32, low / len(cuts), high / len(cuts))
        return jnp.repeat(jnp.exp(steps), dims[dim] // shards_of).reshape((-1,) + (1,) * (len(dims) - dim - 1))

    factor_of = one(*cuts[0])
    for cut in cuts[1:]:
        factor_of = factor_of * one(*cut)
    return factor_of


def noise(own_key, extent, scale, reach, pieces=(), kind=jnp.bfloat16):
    drawn = scale * jax.random.normal(own_key, extent, jnp.float32)
    if pieces:
        drawn = drawn * levels(own_key, extent, pieces, -0.22, 0.18)
    return jnp.clip(drawn, -reach, reach).astype(kind)


def heavy_noise(own_key, shape, width, most, pieces, heavy, held_as=jnp.bfloat16):
    array = width * jax.random.normal(own_key, shape, jnp.float32)
    if pieces:
        array = array * levels(own_key, shape, pieces, -0.22, 0.18)
    return jnp.clip(spiked(array, jax.random.fold_in(own_key, 3), *heavy), -most, most).astype(held_as)


def setup_inputs(seed: int = 0) -> dict:
    seeds = jax.random.split(jax.random.key(seed), 7)
    attn_out = noise(seeds[0], (TOKENS, HD), 1.0, 6.0, ((0, 16), (1, 2)))
    out_proj_t = noise(seeds[1], (D, HD), D ** -0.5, 0.09375, ((1, 2),))
    grad_out = heavy_noise(seeds[2], (TOKENS, D), 1.0, 6.0, ((0, 16), (1, 2)), (0, 1, 16, 2.0))
    read_weights = jnp.clip(0.0026041667 * jax.random.uniform(seeds[3], (TOKENS, MEM), jnp.float32) ** levels(seeds[3], (TOKENS, MEM), ((0, 16),), -0.2, 0.2), 0.0, 0.0026041667)
    memory_gate = draw_memory_gate(jax.random.fold_in(seeds[6], 71), 0)
    write_pos = draw_write_pos(jax.random.fold_in(seeds[6], 71), 0)
    return {"attn_out": attn_out, "out_proj_t": out_proj_t, "grad_out": grad_out, "read_weights": read_weights, "memory_gate": memory_gate, "write_pos": write_pos}


def reference(attn_out, out_proj_t, grad_out, read_weights, memory_gate, write_pos):
    high = lax.Precision.HIGHEST
    dy = grad_out.astype(jnp.float32).reshape(SEGMENT_COUNT, SEG, D)
    reads = read_weights.reshape(SEGMENT_COUNT, SEG, MEM)
    gates = memory_gate.reshape(SEGMENT_COUNT, MEM, MEM)
    local = jnp.einsum('stm,std->smd', reads, dy, precision=high)

    def sweep(carry, inputs):
        gate, term = inputs
        fresh = jnp.dot(gate.T, carry, precision=high, preferred_element_type=jnp.float32) + term
        return fresh, (fresh, carry)

    start = jnp.zeros((MEM, D), jnp.float32)
    _, (grad_mem, after) = lax.scan(sweep, start, (gates, local), reverse=True)
    places = jnp.arange(SEG, dtype=jnp.int32)
    onehot = (places[None, :, None] == write_pos[:, None, :]).astype(jnp.float32)
    written = jnp.einsum('stm,smd->std', onehot, after, precision=high)
    grad_z = (dy + written).astype(jnp.bfloat16).reshape(TOKENS, D)
    grad_attn = jnp.dot(grad_z, out_proj_t, preferred_element_type=jnp.float32).astype(jnp.bfloat16)
    grad_weight = lax.dot_general(grad_z, attn_out, (((0,), (0,)), ((), ())), preferred_element_type=jnp.float32)
    return grad_attn, grad_weight, grad_mem.reshape(SEGMENT_COUNT * MEM, D)
```

```python
import jax
import jax.numpy as jnp
from jax import lax
from jax.sharding import PartitionSpec as P

F32 = jnp.float32
BF16 = jnp.bfloat16


def grid_of(count):
    cores = 2 if count % 2 == 0 else 1
    chips = count // cores
    rows = 1
    while chips % (rows * 2) == 0 and (rows * 2) ** 2 <= chips:
        rows *= 2
    return chips // rows, rows, cores


def cuts_of(rows):
    if rows % 64:
        return [(0, rows)]
    step = rows // 4
    return [(k * step, (k + 1) * step) for k in range(4)]


def body(attn_out, out_proj_t, grad_out, read_weights, memory_gate, write_pos):
    high = lax.Precision.HIGHEST
    seg_len, own_width = grad_out.shape
    heads = attn_out.shape[1]
    slots = write_pos.shape[1]
    count = lax.axis_size("dp")
    parts = lax.axis_size("tensor")
    mine = lax.axis_index("dp")
    side = lax.axis_index("tensor")
    deep, wide, cores = grid_of(count)
    rows = own_width * parts // count
    held = own_width // rows
    pairs = held // cores
    place = (mine // (wide * cores), (mine // cores) % wide, mine % cores)

    def shift_tensor(x, r):
        return lax.ppermute(x, "tensor", [(t, (t + r) % parts) for t in range(parts)])

    def shift_dp(x, axis, r):
        sizes = (deep, wide, cores)
        moves = []
        for i in range(count):
            at = [i // (wide * cores), (i // cores) % wide, i % cores]
            at[axis] = (at[axis] + r) % sizes[axis]
            moves.append((i, (at[0] * wide + at[1]) * cores + at[2]))
        return lax.ppermute(x, "dp", moves)

    cuts = cuts_of(rows)

    def columns(x, lo, hi):
        n = x.shape[0]
        piece = x.reshape(n, pairs, cores, rows)[:, :, :, lo:hi]
        return piece.transpose(0, 2, 1, 3).reshape(n, held * (hi - lo))

    early = (len(cuts) + 1) // 2
    own = [columns(grad_out, lo, hi) for lo, hi in cuts]
    got = [[shift_tensor(x, r) for r in range(1, parts)] for x in own[:early]]

    top = lax.reduce_precision(read_weights, 8, 7)
    rest = read_weights - top
    mid = lax.reduce_precision(rest, 8, 7)
    low = rest - mid
    terms = jnp.concatenate([top, mid, low], axis=1).astype(BF16)
    local3 = lax.dot_general(terms, grad_out, (((0,), (0,)), ((), ())), preferred_element_type=F32)
    local = local3[:slots] + local3[slots : 2 * slots] + local3[2 * slots :]

    gate = memory_gate.T
    lanes = 128 * (-(-slots // 128))
    maps = jnp.concatenate([local, jnp.pad(gate, ((0, 0), (0, lanes - slots)))], axis=1)
    base = jnp.pad(local, ((0, 0), (0, lanes)))

    def later(x, r):
        return lax.ppermute(x, "dp", [(i, i - r) for i in range(r, count)])

    step = 1
    acc = maps
    while step < count:
        come = later(acc, step)
        head = acc[:, own_width : own_width + slots]
        keep = jnp.pad(acc[:, :own_width], ((0, 0), (0, lanes)))
        acc = keep + jnp.dot(head, come, precision=high, preferred_element_type=F32)
        step *= 2
    grad_memory = acc[:, :own_width]
    after = later(grad_memory, 1)

    places = jnp.arange(seg_len, dtype=jnp.int32)
    hits = places[:, None] == write_pos[0][None, :]
    onehot = hits.astype(BF16)
    touched = jnp.any(hits, axis=1)[:, None]
    picked = lax.dot_general(onehot, grad_out, (((0,), (0,)), ((), ())), preferred_element_type=F32)
    fresh = (picked + after).astype(BF16)
    fresh_got = [shift_tensor(fresh, r) for r in range(1, parts)]
    for k in range(early, len(cuts)):
        held_back, _ = lax.optimization_barrier((own[k], fresh))
        got.append([shift_tensor(held_back, r) for r in range(1, parts)])

    def ordered(pieces):
        out = []
        for q in range(parts):
            pick = pieces[0]
            for r in range(1, parts):
                pick = jnp.where((side - r) % parts == q, pieces[r], pick)
            out.append(pick)
        return out

    def reduce_along(x, axis, size):
        here = place[axis]
        total = None
        for r in range(1, size):
            there = lax.dynamic_index_in_dim(x, (here + r) % size, 0, keepdims=False)
            come = shift_dp(there.astype(BF16), axis, r).astype(F32)
            total = come if total is None else total + come
        kept = lax.dynamic_index_in_dim(x, here, 0, keepdims=False)
        return kept if total is None else kept + total

    proj = out_proj_t.reshape(parts, pairs, cores, rows, heads)
    grad_attn = None
    sums = []
    for k, (lo, hi) in enumerate(cuts):
        size = hi - lo
        z_parts = []
        for dy_cut, row_cut in zip(
            ordered([own[k]] + got[k]),
            ordered([columns(x, lo, hi) for x in [fresh] + fresh_got]),
        ):
            put = jnp.dot(onehot, row_cut, preferred_element_type=F32).astype(BF16)
            z_parts.append(jnp.where(touched, put, dy_cut))
        z_cut = jnp.concatenate(z_parts, axis=1)

        def of_core(c):
            take = [
                lax.dynamic_slice_in_dim(x, c * (pairs * size), pairs * size, 1) for x in z_parts
            ]
            lhs = jnp.concatenate(take, axis=1)
            return lax.dot_general(
                lhs, attn_out, (((0,), (0,)), ((), ())), preferred_element_type=F32
            )

        if cores == 2:
            away = of_core(1 - place[2]).astype(BF16)
            part = of_core(place[2]) + shift_dp(away, 2, 1).astype(F32)
        else:
            part = of_core(0)
        part = part.reshape(deep, wide, size, heads)
        part = reduce_along(part.transpose(1, 0, 2, 3), 1, wide)
        sums.append(reduce_along(part, 0, deep))

        w_cut = proj[:, :, :, lo:hi].transpose(0, 2, 1, 3, 4).reshape(-1, heads)
        term = jnp.dot(z_cut, w_cut, preferred_element_type=F32)
        grad_attn = term if grad_attn is None else grad_attn + term
    grad_weight = jnp.concatenate(sums, axis=0)
    return (grad_attn.astype(BF16), grad_weight, grad_memory)


def solution(mesh):
    return jax.shard_map(
        body,
        mesh=mesh,
        in_specs=(
            P("dp", "tensor"),
            P(None, "tensor"),
            P("dp", "tensor"),
            P("dp", None),
            P("dp", None),
            P("dp", None),
        ),
        out_specs=(P("dp", "tensor"), P("dp", "tensor"), P("dp", "tensor")),
        check_vma=False,
    )
```

```python
import jax
import jax.numpy as jnp
from jax import lax
from jax.sharding import PartitionSpec as P

F32 = jnp.float32
BF16 = jnp.bfloat16


def grid_of(count):
    cores = 2 if count % 2 == 0 else 1
    chips = count // cores
    rows = 1
    while chips % (rows * 2) == 0 and (rows * 2) ** 2 <= chips:
        rows *= 2
    return chips // rows, rows, cores


def cuts_of(rows):
    if rows % 128 or rows == 128:
        return [(0, rows)]
    return [(0, rows // 2), (rows // 2, rows)]


def body(attn_out, out_proj_t, grad_out, read_weights, memory_gate, write_pos):
    high = lax.Precision.HIGHEST
    seg_len, own_width = grad_out.shape
    heads = attn_out.shape[1]
    slots = write_pos.shape[1]
    count = lax.axis_size("dp")
    parts = lax.axis_size("tensor")
    mine = lax.axis_index("dp")
    side = lax.axis_index("tensor")
    deep, wide, cores = grid_of(count)
    rows = own_width * parts // count
    held = own_width // rows
    pairs = held // cores
    place = (mine // (wide * cores), (mine // cores) % wide, mine % cores)

    def shift_tensor(x, r):
        return lax.ppermute(x, "tensor", [(t, (t + r) % parts) for t in range(parts)])

    def shift_dp(x, axis, move):
        moves = []
        for i in range(count):
            at = [i // (wide * cores), (i // cores) % wide, i % cores]
            at[axis] = move(at[axis])
            moves.append((i, (at[0] * wide + at[1]) * cores + at[2]))
        return lax.ppermute(x, "dp", moves)

    cuts = cuts_of(rows)

    def columns(x, lo, hi):
        return jnp.concatenate(
            [
                x[:, (p * cores + c) * rows + lo : (p * cores + c) * rows + hi]
                for c in range(cores)
                for p in range(pairs)
            ],
            axis=1,
        )

    own = [columns(grad_out, lo, hi) for lo, hi in cuts]
    got = [[shift_tensor(own[0], r) for r in range(1, parts)]]

    top = lax.reduce_precision(read_weights, 8, 7)
    rest = read_weights - top
    mid = lax.reduce_precision(rest, 8, 7)
    low = rest - mid
    terms = jnp.concatenate([top, mid, low], axis=1).astype(BF16)
    local3 = lax.dot_general(terms, grad_out, (((0,), (0,)), ((), ())), preferred_element_type=F32)
    local = local3[:slots] + local3[slots : 2 * slots] + local3[2 * slots :]

    gate = memory_gate.T
    lanes = 128 * (-(-slots // 128))
    maps = jnp.concatenate([local, jnp.pad(gate, ((0, 0), (0, lanes - slots)))], axis=1)
    base = jnp.pad(local, ((0, 0), (0, lanes)))

    def later(x, r):
        return lax.ppermute(x, "dp", [(i, i - r) for i in range(r, count)])

    step = 1
    acc = maps
    while step < count:
        come = later(acc, step)
        head = acc[:, own_width : own_width + slots]
        keep = jnp.pad(acc[:, :own_width], ((0, 0), (0, lanes)))
        acc = keep + jnp.dot(head, come, precision=high, preferred_element_type=F32)
        step *= 2
    grad_memory = acc[:, :own_width]
    after = later(grad_memory, 1)

    places = jnp.arange(seg_len, dtype=jnp.int32)
    hits = places[:, None] == write_pos[0][None, :]
    onehot = hits.astype(BF16)
    touched = jnp.any(hits, axis=1)[:, None]
    picked = lax.dot_general(onehot, grad_out, (((0,), (0,)), ((), ())), preferred_element_type=F32)
    fresh = (picked + after).astype(BF16)
    fresh_got = [shift_tensor(fresh, r) for r in range(1, parts)]
    for k in range(1, len(cuts)):
        got.append([shift_tensor(own[k], r) for r in range(1, parts)])

    def ordered(pieces):
        out = []
        for q in range(parts):
            pick = pieces[0]
            for r in range(1, parts):
                pick = jnp.where((side - r) % parts == q, pieces[r], pick)
            out.append(pick)
        return out

    def put_rows(dy_cut, row_cut):
        put = jnp.dot(onehot, row_cut, preferred_element_type=F32).astype(BF16)
        return jnp.where(touched, put, dy_cut)

    def near_sum(z_cut, size):
        width = pairs * size

        def of_core(c):
            lhs = lax.dynamic_slice_in_dim(z_cut, c * width, width, 1)
            return lax.dot_general(
                lhs, attn_out, (((0,), (0,)), ((), ())), preferred_element_type=F32
            )

        if cores == 2:
            away = of_core(1 - place[2]).astype(BF16)
            part = of_core(place[2])
            part = part + shift_dp(away, 2, lambda v: 1 - v).astype(F32)
        else:
            part = of_core(0)
        part = part.reshape(pairs // wide, wide, size, heads)
        here = place[1]
        total = lax.dynamic_index_in_dim(part, here, 1, keepdims=False)
        for r in range(1, wide):
            there = lax.dynamic_index_in_dim(part, (here + r) % wide, 1, keepdims=False)
            come = shift_dp(there.astype(BF16), 1, lambda v: (v + r) % wide)
            total = total + come.astype(F32)
        return total

    def deep_sum(x):
        bit = 1
        while bit < deep:
            x = x.reshape((x.shape[0] // 2, 2) + x.shape[1:])
            here = (place[0] // bit) % 2
            away = lax.dynamic_index_in_dim(x, 1 - here, 1, keepdims=False).astype(BF16)
            come = shift_dp(away, 0, lambda v: v ^ bit)
            x = lax.dynamic_index_in_dim(x, here, 1, keepdims=False) + come.astype(F32)
            bit *= 2
        return x[0]

    proj = out_proj_t.reshape(parts, pairs, cores, rows, heads)
    z_own, near_own, row_cuts = [], [], []
    for k, (lo, hi) in enumerate(cuts):
        row_cuts.append([columns(x, lo, hi) for x in [fresh] + fresh_got])
        z_own.append(put_rows(own[k], row_cuts[k][0]))
        near_own.append(near_sum(z_own[k], hi - lo))
    grad_attn = None
    sums = []
    for k, (lo, hi) in enumerate(cuts):
        z_got = [put_rows(x, y) for x, y in zip(got[k], row_cuts[k][1:])]
        near = [near_own[k]] + [near_sum(z, hi - lo) for z in z_got]
        sums.append(deep_sum(jnp.concatenate(ordered(near), axis=0)))
        w_cut = proj[:, :, :, lo:hi].transpose(0, 2, 1, 3, 4).reshape(parts, -1, heads)
        for r, z in enumerate([z_own[k]] + z_got):
            w = lax.dynamic_index_in_dim(w_cut, (side - r) % parts, 0, keepdims=False)
            term = jnp.dot(z, w, preferred_element_type=F32)
            grad_attn = term if grad_attn is None else grad_attn + term
    grad_weight = jnp.concatenate(sums, axis=0)
    return (grad_attn.astype(BF16), grad_weight, grad_memory)


def solution(mesh):
    return jax.shard_map(
        body,
        mesh=mesh,
        in_specs=(
            P("dp", "tensor"),
            P(None, "tensor"),
            P("dp", "tensor"),
            P("dp", None),
            P("dp", None),
            P("dp", None),
        ),
        out_specs=(P("dp", "tensor"), P("dp", "tensor"), P("dp", "tensor")),
        check_vma=False,
    )
```

```python
import jax
import jax.numpy as jnp
from jax import lax
from jax.experimental import pallas as pl
from jax.sharding import PartitionSpec as P

F32 = jnp.float32
BF16 = jnp.bfloat16


def grid_of(count):
    cores = 2 if count % 2 == 0 else 1
    chips = count // cores
    rows = 1
    while chips % (rows * 2) == 0 and (rows * 2) ** 2 <= chips:
        rows *= 2
    return chips // rows, rows, cores


def cuts_of(rows):
    if rows % 128 or rows == 128:
        return [(0, rows)]
    return [(0, rows // 2), (rows // 2, rows)]


def copy_block(src, dst):
    dst[...] = src[...]


def body(attn_out, out_proj_t, grad_out, read_weights, memory_gate, write_pos):
    high = lax.Precision.HIGHEST
    seg_len, own_width = grad_out.shape
    heads = attn_out.shape[1]
    slots = write_pos.shape[1]
    count = lax.axis_size("dp")
    parts = lax.axis_size("tensor")
    mine = lax.axis_index("dp")
    side = lax.axis_index("tensor")
    deep, wide, cores = grid_of(count)
    rows = own_width * parts // count
    held = own_width // rows
    pairs = held // cores
    place = (mine // (wide * cores), (mine // cores) % wide, mine % cores)

    def shift_tensor(x, r):
        return lax.ppermute(x, "tensor", [(t, (t + r) % parts) for t in range(parts)])

    def shift_dp(x, axis, move):
        moves = []
        for i in range(count):
            at = [i // (wide * cores), (i // cores) % wide, i % cores]
            at[axis] = move(at[axis])
            moves.append((i, (at[0] * wide + at[1]) * cores + at[2]))
        return lax.ppermute(x, "dp", moves)

    cuts = cuts_of(rows)

    def columns(x, lo, hi):
        size = hi - lo
        n = x.shape[0]
        if size % 128 == 0:
            per = rows // size
            return pl.pallas_call(
                copy_block,
                grid=(cores, pairs),
                in_specs=[
                    pl.BlockSpec(
                        (n, size), lambda c, p: (0, (p * cores + c) * per + lo // size)
                    )
                ],
                out_specs=pl.BlockSpec((n, size), lambda c, p: (0, c * pairs + p)),
                out_shape=jax.ShapeDtypeStruct((n, held * size), x.dtype),
            )(x)
        return jnp.concatenate(
            [
                x[:, (p * cores + c) * rows + lo : (p * cores + c) * rows + hi]
                for c in range(cores)
                for p in range(pairs)
            ],
            axis=1,
        )

    own = [columns(grad_out, lo, hi) for lo, hi in cuts]
    got = [[shift_tensor(own[0], r) for r in range(1, parts)]]

    top = lax.reduce_precision(read_weights, 8, 7)
    rest = read_weights - top
    mid = lax.reduce_precision(rest, 8, 7)
    low = rest - mid
    terms = jnp.concatenate([top, mid, low], axis=1).astype(BF16)
    local3 = lax.dot_general(terms, grad_out, (((0,), (0,)), ((), ())), preferred_element_type=F32)
    local = local3[:slots] + local3[slots : 2 * slots] + local3[2 * slots :]

    gate = memory_gate.T
    lanes = 128 * (-(-slots // 128))
    maps = jnp.concatenate([local, jnp.pad(gate, ((0, 0), (0, lanes - slots)))], axis=1)
    base = jnp.pad(local, ((0, 0), (0, lanes)))

    def later(x, r):
        return lax.ppermute(x, "dp", [(i, i - r) for i in range(r, count)])

    step = 1
    acc = maps
    while step < count:
        come = later(acc, step)
        head = acc[:, own_width : own_width + slots]
        keep = jnp.pad(acc[:, :own_width], ((0, 0), (0, lanes)))
        acc = keep + jnp.dot(head, come, precision=high, preferred_element_type=F32)
        step *= 2
    grad_memory = acc[:, :own_width]
    after = later(grad_memory, 1)

    places = jnp.arange(seg_len, dtype=jnp.int32)
    hits = places[:, None] == write_pos[0][None, :]
    onehot = hits.astype(BF16)
    touched = jnp.any(hits, axis=1)[:, None]
    picked = lax.dot_general(onehot, grad_out, (((0,), (0,)), ((), ())), preferred_element_type=F32)
    fresh = (picked + after).astype(BF16)
    fresh_got = [shift_tensor(fresh, r) for r in range(1, parts)]
    for k in range(1, len(cuts)):
        got.append([shift_tensor(own[k], r) for r in range(1, parts)])

    def ordered(pieces):
        out = []
        for q in range(parts):
            pick = pieces[0]
            for r in range(1, parts):
                pick = jnp.where((side - r) % parts == q, pieces[r], pick)
            out.append(pick)
        return out

    def put_rows(dy_cut, row_cut):
        put = jnp.dot(onehot, row_cut, preferred_element_type=F32).astype(BF16)
        return jnp.where(touched, put, dy_cut)

    def near_sum(z_cut, size):
        width = pairs * size

        def of_core(c):
            lhs = lax.dynamic_slice_in_dim(z_cut, c * width, width, 1)
            return lax.dot_general(
                lhs, attn_out, (((0,), (0,)), ((), ())), preferred_element_type=F32
            )

        if cores == 2:
            away = of_core(1 - place[2]).astype(BF16)
            part = of_core(place[2])
            part = part + shift_dp(away, 2, lambda v: 1 - v).astype(F32)
        else:
            part = of_core(0)
        part = part.reshape(pairs // wide, wide, size, heads)
        here = place[1]
        total = lax.dynamic_index_in_dim(part, here, 1, keepdims=False)
        for r in range(1, wide):
            there = lax.dynamic_index_in_dim(part, (here + r) % wide, 1, keepdims=False)
            come = shift_dp(there.astype(BF16), 1, lambda v: (v + r) % wide)
            total = total + come.astype(F32)
        return total

    def deep_sum(x):
        bit = 1
        while bit < deep:
            x = x.reshape((x.shape[0] // 2, 2) + x.shape[1:])
            here = (place[0] // bit) % 2
            away = lax.dynamic_index_in_dim(x, 1 - here, 1, keepdims=False).astype(BF16)
            come = shift_dp(away, 0, lambda v: v ^ bit)
            x = lax.dynamic_index_in_dim(x, here, 1, keepdims=False) + come.astype(F32)
            bit *= 2
        return x[0]

    def rows_of(lo, hi):
        size = hi - lo
        per = rows // size
        return pl.pallas_call(
            copy_block,
            grid=(parts, cores, pairs),
            in_specs=[
                pl.BlockSpec(
                    (size, heads),
                    lambda t, c, p: (((t * pairs + p) * cores + c) * per + lo // size, 0),
                )
            ],
            out_specs=pl.BlockSpec(
                (size, heads), lambda t, c, p: ((t * cores + c) * pairs + p, 0)
            ),
            out_shape=jax.ShapeDtypeStruct((parts * held * size, heads), out_proj_t.dtype),
        )(out_proj_t)

    z_own, near_own, row_cuts = [], [], []
    for k, (lo, hi) in enumerate(cuts):
        row_cuts.append([columns(x, lo, hi) for x in [fresh] + fresh_got])
        z_own.append(put_rows(own[k], row_cuts[k][0]))
        near_own.append(near_sum(z_own[k], hi - lo))
    grad_attn = None
    sums = []
    for k, (lo, hi) in enumerate(cuts):
        z_got = [put_rows(x, y) for x, y in zip(got[k], row_cuts[k][1:])]
        near = [near_own[k]] + [near_sum(z, hi - lo) for z in z_got]
        sums.append(deep_sum(jnp.concatenate(ordered(near), axis=0)))
        w_cut = rows_of(lo, hi).reshape(parts, -1, heads)
        for r, z in enumerate([z_own[k]] + z_got):
            w = lax.dynamic_index_in_dim(w_cut, (side - r) % parts, 0, keepdims=False)
            term = jnp.dot(z, w, preferred_element_type=F32)
            grad_attn = term if grad_attn is None else grad_attn + term
    grad_weight = jnp.concatenate(sums, axis=0)
    return (grad_attn.astype(BF16), grad_weight, grad_memory)


def solution(mesh):
    return jax.shard_map(
        body,
        mesh=mesh,
        in_specs=(
            P("dp", "tensor"),
            P(None, "tensor"),
            P("dp", "tensor"),
            P("dp", None),
            P("dp", None),
            P("dp", None),
        ),
        out_specs=(P("dp", "tensor"), P("dp", "tensor"), P("dp", "tensor")),
        check_vma=False,
    )
```
